128 devices in a mesh: row: 8 (over z, core), col: 16 (over y, x).
Axes of the slice: x: 4, y: 4, z: 4, core: 2. Of those that a mesh axis runs over, the one named last changes fastest.
Arguments:
- real_feats: bfloat16 [16384, 2048], P(('row', 'col')), may hold values from 0 to 8, as said below
- fake_feats: bfloat16 [16384, 2048], P(('row', 'col')), may hold values from 0 to 8, as said below
Outputs:
- proof_real: float32 [16384], P(('row', 'col'))
- proof_fake: float32 [16384], P(('row', 'col'))
- kid: float32 [], replicated
The draws below stay inside these ranges and needn't reach their ends.
Inputs may be any that keep to these rules, and one draw needn't show every extreme that they name: `real_feats`: nonnegative features. `fake_feats`: nonnegative features.
All inputs are finite; a program needn't handle non-finite values.
Results may differ from the reference program's by a relative error of at most 0.0003.
Values may be sent and summed in bfloat16 or wider, within the bound.
No kernel may reach another device: no remote copies, remote signals or barrier semaphores. Data moves between devices by JAX's collectives and lax.ppermute only.
A program may use at most 128 MiB of HBM per device.

```python
import math
import jax
import jax.numpy as jnp
from jax import lax

D = 2048
M = 16384


centroid_count = 1000


value_top = 8.0


def centroid_table(key):
    first, second = jax.random.split(jax.random.fold_in(key, 5))
    values = 2.0 * jnp.exp(1.2 * jax.random.normal(first, (centroid_count, D), jnp.float32))
    active = jax.random.uniform(second, (centroid_count, D), jnp.float32) < 0.2
    return jnp.where(active, values, 0.0)


def make_features(key, which, ramp_low, tilt_spread):
    table = centroid_table(key)
    keys = jax.random.split(jax.random.fold_in(key, 17 + which), 8)
    picks = jax.random.randint(keys[0], (M, 3), 0, centroid_count, dtype=jnp.int32)
    weights = jax.random.uniform(keys[1], (M, 3), jnp.float32, 0.2, 1.0)
    keep_third = (jax.random.uniform(keys[2], (M, 1), jnp.float32) < 0.5).astype(jnp.float32)
    weights = weights * jnp.concatenate([jnp.ones((M, 2), jnp.float32), keep_third], axis=1)
    weights = weights / jnp.sum(weights, axis=1, keepdims=True)
    labels = jnp.arange(centroid_count, dtype=jnp.int32)
    mixing = jnp.zeros((M, centroid_count), jnp.float32)
    for slot in range(3):
        mixing = mixing + jnp.where(picks[:, slot:slot + 1] == labels[None, :], weights[:, slot:slot + 1], 0.0)
    mixed = jnp.dot(mixing, table, precision=lax.Precision.HIGHEST)
    tilt = jnp.exp(tilt_spread * jax.random.uniform(jax.random.fold_in(key, 29), (1, D), jnp.float32, -1.0, 1.0))
    mixed = mixed * tilt
    noise = 0.3 * jax.random.uniform(keys[3], (M, D), jnp.float32)
    noise = jnp.where(jax.random.uniform(keys[4], (M, D), jnp.float32) < 0.5, noise, 0.0)
    base = mixed + noise
    position = jnp.arange(M, dtype=jnp.float32) / M
    jitter = jax.random.uniform(keys[7], (M, 1), jnp.float32, -0.4, 0.4)
    scales = jnp.exp(jitter) * (ramp_low + 2.0 * ramp_low * position)[:, None]
    return jnp.minimum(scales * base, value_top).astype(jnp.bfloat16)


def draw_real_feats(key, part):
    return make_features(key, 0, 0.5, 0.0)


def draw_fake_feats(key, part):
    return make_features(key, 1, 0.45, 0.5)


def setup_inputs(seed: int = 0) -> dict:
    streams_of = jax.random.split(jax.random.key(seed), 3)
    real_feats = draw_real_feats(jax.random.fold_in(streams_of[2], 71), 0)
    fake_feats = draw_fake_feats(jax.random.fold_in(streams_of[2], 71), 0)
    return {"real_feats": real_feats, "fake_feats": fake_feats}


def kernel_block(left, right):
    inner = lax.dot_general(left, right, (((1,), (1,)), ((), ())), preferred_element_type=jnp.float32)
    shifted = inner / D + 1.0
    return shifted * shifted * shifted


def reference(real_feats, fake_feats):
    total = real_feats.shape[0]
    step = math.gcd(total, 512)
    count = total // step
    every = jnp.arange(total, dtype=jnp.int32)

    def one_block(index):
        start = (index * step).astype(jnp.int32)
        left_real = lax.dynamic_slice_in_dim(real_feats, start, step, 0)
        left_fake = lax.dynamic_slice_in_dim(fake_feats, start, step, 0)
        own = start + jnp.arange(step, dtype=jnp.int32)
        off_diag = own[:, None] != every[None, :]
        same_real = jnp.where(off_diag, kernel_block(left_real, real_feats), 0.0)
        same_fake = jnp.where(off_diag, kernel_block(left_fake, fake_feats), 0.0)
        cross_real = kernel_block(left_real, fake_feats)
        cross_fake = kernel_block(left_fake, real_feats)
        first = jnp.sum(same_real, axis=1) / (total - 1.0) - jnp.sum(cross_real, axis=1) / total
        second = jnp.sum(same_fake, axis=1) / (total - 1.0) - jnp.sum(cross_fake, axis=1) / total
        return first, second

    firsts, seconds = lax.map(one_block, jnp.arange(count, dtype=jnp.int32))
    proof_real = firsts.reshape(total)
    proof_fake = seconds.reshape(total)
    kid = (jnp.sum(proof_real) + jnp.sum(proof_fake)) / total
    return proof_real, proof_fake, kid
```

```python
import functools

import numpy as np

import jax
import jax.numpy as jnp
from jax import lax
from jax.experimental import pallas as pl
from jax.experimental.pallas import tpu as pltpu
from jax.sharding import PartitionSpec as P

AXES = ("row", "col")
STEPS = ((1, 0, 0), (3, 0, 0), (0, 1, 0), (0, 3, 0), (0, 0, 1), (0, 0, 3))

HOPS = (
    (0, 0, 4, 3),
    (0, 0, 0, 5),
    (0, 0, 1, 2),
    (1, 0, 3, 0),
    (2, 1, 1, 5),
    (3, 1, 4, 2),
    (4, 1, 5, 3),
    (4, 0, 0, 4),
    (5, 0, 2, 0),
    (5, 1, 1, 3),
    (6, 1, 4, 2),
    (7, 0, 5, 1),
)

FIRST = (0, 0, 0, 0, 1, 1, 2, 2, 2, 3, 3, 3, 3)
FIRST_SWAPPED = (0, 0, 0, 1, 1, 2, 2, 2, 3, 3, 3, 3, 3)
TILES = (16,24,24,64,)

WIDTH = 2048
ROWS = 16384
UNROLL = 8


def plus(a, b):
    return tuple((p + q) % 4 for p, q in zip(a, b))


def minus(a, b):
    return tuple((p - q) % 4 for p, q in zip(a, b))


def device_of(chip, core):
    x, y, z = chip
    return (z * 2 + core) * 16 + y * 4 + x


CHIPS = [(x, y, z) for z in range(4) for y in range(4) for x in range(4)]


def items_of_variables():
    origin = (0, 0, 0)
    held = [((origin, 0), (origin, 1))]
    for source, swapped, step0, step1 in HOPS:
        pair = held[source][::-1] if swapped else held[source]
        held.append(
            tuple((plus(t, STEPS[s]), h) for (t, h), s in zip(pair, (step0, step1)))
        )
    return held


def make_plan():
    held = items_of_variables()
    count = 2 * len(held)
    item = [[held[a // 2][q ^ (a % 2)] for a in range(count)] for q in range(2)]
    first = [0] * count
    for v in range(len(held)):
        first[2 * v], first[2 * v + 1] = FIRST[v], FIRST_SWAPPED[v]
    ways = {}
    for q in range(2):
        for a in range(count):
            for b in range(count):
                if a != b and first[a] < 99 and first[b] < 99:
                    (t, h), (s, g) = item[q][a], item[q][b]
                    key = (minus(t, s), h, g)
                    ways.setdefault(key, [[], []])[q].append((max(first[a], first[b]), a, b))
    tasks = []
    for delta in CHIPS:
        back = minus((0, 0, 0), delta)
        if delta == (0, 0, 0) or back < delta:
            continue
        if back == delta:
            dim = [i for i in range(3) if delta[i]][0]
            both = []
            for q in range(2):
                low = sorted(ways[(delta, 0, 0)][q])
                high = sorted(ways[(delta, 1, 1)][q])
                pick = []
                for w0 in low:
                    for w1 in high:
                        pick.append((max(w0[0], w1[0]), (w0[1:], w1[1:]), dim))
                both.append(sorted(pick))
            tasks.append(both)
            kinds = [(0, 1)]
        else:
            kinds = [(0, 0), (0, 1), (1, 0), (1, 1)]
        for h, g in kinds:
            both = []
            for q in range(2):
                both.append(
                    sorted((p, ((a, b), (a, b)), 0) for p, a, b in ways[(delta, h, g)][q])
                )
            tasks.append(both)
    done = [False] * len(tasks)
    phases = []
    for p, room in enumerate(TILES):
        lists = [[], []]
        while True:
            q = 0 if len(lists[0]) <= len(lists[1]) else 1
            placed = False
            for core in (q, 1 - q):
                if len(lists[core]) >= room:
                    continue
                best = None
                for k, both in enumerate(tasks):
                    if done[k]:
                        continue
                    mine = [w for w in both[core] if w[0] <= p]
                    if not mine:
                        continue
                    other = [w for w in both[1 - core] if w[0] <= p]
                    rank = (len(other) > 0, -mine[-1][0], len(mine))
                    if best is None or rank < best[0]:
                        best = (rank, k, mine)
                if best is not None:
                    _, k, mine = best
                    done[k] = True
                    used = set()
                    for w in lists[core]:
                        used.update(w[1][0] + w[1][1])
                    fewest = min(mine, key=lambda w: len(set(w[1][0] + w[1][1]) - used))
                    lists[core].append(fewest)
                    placed = True
                    break
            if not placed:
                break
        phases.append(lists)
    assert all(done)
    return item, phases


def order_arrays(lists, start):
    names = sorted({a for side in lists for w in side for pair in w[1] for a in pair} | set(start))
    placed = list(start)
    while len(placed) < len(names):
        def score(a):
            have = set(placed) | {a}
            return sum(
                all(x in have for pair in w[1] for x in pair) for side in lists for w in side
            )
        placed.append(max((a for a in names if a not in placed), key=score))
    return placed


def make_tables():
    item, phases = make_plan()
    layout = []
    width = 0
    for p, lists in enumerate(phases):
        arrays = order_arrays(lists, [0, 1] if p == 0 else [])
        tiles = max(len(side) for side in lists)
        tiles = -(-tiles // UNROLL) * UNROLL
        layout.append((arrays, tiles, width))
        width += 4 * tiles + tiles // UNROLL
    owners_at = width
    width += len(item[0])
    table = np.zeros((128, width), np.int32)
    for chip in CHIPS:
        for q in range(2):
            line = table[device_of(chip, q)]
            for (arrays, tiles, at), lists in zip(layout, phases):
                place = {a: i for i, a in enumerate(arrays)}
                picked = []
                for _, pairs, dim in lists[q]:
                    a, b = pairs[chip[dim] // 2]
                    picked.append((place[a], place[b]))
                picked.sort(key=max)
                trash = len(arrays)
                for u in range(tiles):
                    if u < len(picked):
                        a, b = picked[u]
                        line[at + 4 * u : at + 4 * u + 4] = (a, b, a, b)
                    else:
                        line[at + 4 * u : at + 4 * u + 4] = (0, 0, trash, trash)
                for v in range(tiles // UNROLL):
                    part = picked[: (v + 1) * UNROLL]
                    line[at + 4 * tiles + v] = 1 + max([max(ab) for ab in part] + [0])
            for a, (t, h) in enumerate(item[q]):
                line[owners_at + a] = device_of(plus(chip, t), h)
    return layout, owners_at, table


def cubed(left, right):
    inner = lax.dot_general(
        left, right, (((1,), (1,)), ((), ())), preferred_element_type=jnp.float32
    )
    shifted = inner + float(WIDTH)
    return shifted * shifted * shifted


def tile_kernel(phase, layout, owners_at, total, *refs):
    arrays, tiles, at = layout[phase]
    last = phase == len(layout) - 1
    n = len(arrays)
    table = refs[0]
    sources = refs[1 : 1 + n]
    earlier = refs[1 + n : 1 + n + phase] if last else ()
    out, rows, row_sums, col_sums, sems = refs[-5:]
    for i in range(n):
        pltpu.make_async_copy(sources[i], rows.at[i], sems.at[i]).start()
    row_sums[...] = jnp.zeros_like(row_sums)
    col_sums[...] = jnp.zeros_like(col_sums)

    def wait_for(i, carry):
        pltpu.make_async_copy(sources[0], rows.at[i], sems.at[i]).wait()
        return carry

    def add_rows(i, p):
        row_sums[i, 0] += p[:, :128]
        row_sums[i, 1] += p[:, 128:]

    ready = 0
    if phase == 0:
        ready = 2
        lax.fori_loop(0, 2, wait_for, 0)
        left = rows[0]
        p = cubed(left, left)
        i0 = lax.broadcasted_iota(jnp.int32, p.shape, 0)
        i1 = lax.broadcasted_iota(jnp.int32, p.shape, 1)
        add_rows(0, jnp.where(i0 == i1, 0.0, p))
        add_rows(0, cubed(left, rows[1]))

    def some_tiles(v, ready):
        need = jnp.maximum(table[at + 4 * tiles + v], ready)
        lax.fori_loop(ready, need, wait_for, 0)
        for j in range(UNROLL):
            u = at + 4 * (v * UNROLL + j)
            p = cubed(rows[table[u]], rows[table[u + 1]])
            add_rows(table[u + 2], p)
            c = table[u + 3]
            col_sums[c, 0] += jnp.sum(p[:128].reshape(16, 8, 256), axis=0)
            col_sums[c, 1] += jnp.sum(p[128:].reshape(16, 8, 256), axis=0)
        return need

    ready = lax.fori_loop(0, tiles // UNROLL, some_tiles, jnp.int32(ready))
    lax.fori_loop(ready, n, wait_for, 0)

    same = 1.0 / ((ROWS - 1.0) * WIDTH**3)
    cross = -1.0 / (float(ROWS) * WIDTH**3)
    sums = {}
    for i, a in enumerate(arrays):
        r0, r1 = row_sums[i, 0], row_sums[i, 1]
        r = jnp.concatenate(
            [same * r0[:128] + cross * r1[:128], cross * r0[128:] + same * r1[128:]], axis=0
        )
        c0, c1 = col_sums[i, 0], col_sums[i, 1]
        c = jnp.concatenate(
            [
                same * c0[:, :128] + cross * c1[:, :128],
                cross * c0[:, 128:] + same * c1[:, 128:],
            ],
            axis=1,
        )
        eight = jnp.sum(r.T.reshape(16, 8, 256), axis=0) + c
        sums[a] = jnp.sum(eight, axis=0, keepdims=True)
    if not last:
        out[...] = jnp.zeros_like(out)
        for a in arrays:
            out[a : a + 1, :] = sums[a]
        return
    out[...] = jnp.zeros_like(out)
    everything = jnp.zeros((1, 128), jnp.float32)
    for a in range(total):
        s = sums.get(a, jnp.zeros((1, 256), jnp.float32))
        for e in earlier:
            s = s + e[a : a + 1, :]
        everything = everything + s[:, :128] + s[:, 128:]
        out[pl.ds(table[owners_at + a], 1), 0:256] = s
    out[:, 256:384] = jnp.broadcast_to(everything, (128, 128))


def run_phase(phase, layout, owners_at, total, table, values, earlier):
    arrays, tiles, _ = layout[phase]
    last = phase == len(layout) - 1
    n = len(arrays)
    vmem = pl.BlockSpec(memory_space=pltpu.VMEM)
    shape = (128, 384) if last else (-(-total // 8) * 8, 256)
    return pl.pallas_call(
        functools.partial(tile_kernel, phase, layout, owners_at, total),
        out_shape=jax.ShapeDtypeStruct(shape, jnp.float32),
        in_specs=[pl.BlockSpec(memory_space=pltpu.SMEM)]
        + [pl.BlockSpec(memory_space=pl.ANY)] * n
        + [vmem] * (phase if last else 0),
        out_specs=vmem,
        scratch_shapes=[
            pltpu.VMEM((n, 256, WIDTH), jnp.bfloat16),
            pltpu.VMEM((n + 1, 2, 256, 128), jnp.float32),
            pltpu.VMEM((n + 1, 2, 8, 256), jnp.float32),
            pltpu.SemaphoreType.DMA((n,)),
        ],
        compiler_params=pltpu.CompilerParams(vmem_limit_bytes=56 * 2**20),
        cost_estimate=pl.CostEstimate(
            flops=tiles * 2 * 256 * 256 * WIDTH, bytes_accessed=n * 2**20, transcendentals=0
        ),
        name=f"tiles{phase}",
    )(table, *[values[a] for a in arrays], *(earlier if last else ()))


def hop(value, step0, step1):
    pairs = []
    for chip in CHIPS:
        for q, s in enumerate((step0, step1)):
            pairs.append((device_of(plus(chip, STEPS[s]), q), device_of(chip, q)))
    return lax.ppermute(value, AXES, pairs)


def swap(value):
    return lax.ppermute(
        value, AXES, [(device_of(c, q), device_of(c, 1 - q)) for c in CHIPS for q in range(2)]
    )


def shards(layout, owners_at, table, real_feats, fake_feats):
    me = lax.axis_index(AXES)
    mine = lax.dynamic_index_in_dim(jnp.asarray(table), me, 0, keepdims=False)
    own = jnp.concatenate([real_feats, fake_feats], axis=0)
    needed = {a for arrays, _, _ in layout for a in arrays}
    needed |= {2 * s + 1 for s, w, _, _ in HOPS if w}
    values = {0: own}
    if 1 in needed:
        values[1] = swap(own)
    for k, (source, swapped, step0, step1) in enumerate(HOPS):
        values[2 * k + 2] = hop(values[2 * source + swapped], step0, step1)
        if 2 * k + 3 in needed:
            values[2 * k + 3] = swap(values[2 * k + 2])
    total = 2 * len(HOPS) + 2
    parts = []
    for phase in range(len(layout)):
        parts.append(run_phase(phase, layout, owners_at, total, mine, values, parts))
    received = lax.all_to_all(parts[-1], AXES, 0, 0, tiled=True)
    sums = jnp.sum(received, axis=0)
    return sums[:128], sums[128:256], jnp.sum(sums[256:]) / float(ROWS)


def solution(mesh):
    layout, owners_at, table = make_tables()
    placed = P(AXES, None)
    return jax.shard_map(
        functools.partial(shards, layout, owners_at, table),
        mesh=mesh,
        in_specs=(placed, placed),
        out_specs=(P(AXES), P(AXES), P()),
        check_vma=False,
    )
```

```python
import functools

import numpy as np

import jax
import jax.numpy as jnp
from jax import lax
from jax.experimental import pallas as pl
from jax.experimental.pallas import tpu as pltpu
from jax.sharding import PartitionSpec as P


AXES = ("row", "col")
STEPS = (1, 3, 4, 12, 16, 48)

GROUP = (
    (2, 1, 0, 1, 1, 1, 2, 1, 3),
    (0, 1, 2, 1, 1, 1, 2, 2, 1),
)

HOPS = (
    (0, 0, 4, 0),
    (0, 0, 3, 2),
    (0, 1, 1, 5),
    (0, 1, 4, 0),
    (0, 1, 3, 2),
    (2, 0, 1, 5),
    (3, 0, 1, 5),
    (4, 0, 4, 0),
    (1, 0, 3, 2),
    (5, 1, 4, 0),
    (6, 0, 1, 5),
    (8, 0, 3, 2),
)

FIRST = (0, 0, 0, 0, 0, 1, 1, 1, 1, 1, 2, 2, 2)
FIRST_SWAPPED = (0, 0, 0, 0, 1, 1, 1, 2, 2, 2, 2, 2, 2)
TILES = (24, 24, 64)

WIDTH = 2048
ROWS = 16384
UNROLL = 8


def group_table():
    def apply(f, v):
        c = (v % 4, v // 4 % 4, v // 16)
        return sum((f[3 + i] * c[f[i]] + f[6 + i]) % 4 * 4**i for i in range(3))

    start = tuple(range(64))
    gens = [tuple(apply(f, v) for v in range(64)) for f in GROUP]
    found, queue = {start}, [start]
    while queue:
        m = queue.pop()
        for g in gens:
            new = tuple(g[v] for v in m)
            if new not in found:
                found.add(new)
                queue.append(new)
    table = {m[0]: m for m in found}
    assert len(found) == len(table) == 64
    return [table[g] for g in range(64)]


M = group_table()
INVERSE = [M[g].index(0) for g in range(64)]
CHIPS = range(64)


def device_of(chip, core):
    return (chip // 16 * 2 + core) * 16 + chip % 16


def items_of_variables():
    held = [((0, 0), (0, 1))]
    for source, swapped, step0, step1 in HOPS:
        pair = held[source][::-1] if swapped else held[source]
        held.append(
            tuple((M[STEPS[s]][t], h) for (t, h), s in zip(pair, (step0, step1)))
        )
    return held


def make_tasks(item, first):
    ways = {}
    for q in range(2):
        for a in range(len(first)):
            for b in range(len(first)):
                if a != b:
                    (t, h), (s, g) = item[q][a], item[q][b]
                    key = (M[INVERSE[t]][s], h, g)
                    ways.setdefault(key, [[], []])[q].append((max(first[a], first[b]), a, b))
    tasks = []
    for delta in range(1, 64):
        if INVERSE[delta] < delta:
            continue
        if INVERSE[delta] == delta:
            both = []
            for q in range(2):
                pick = []
                for p0, a, b in ways[(delta, 0, 0)][q]:
                    for p1, c, d in ways[(delta, 1, 1)][q]:
                        t, s, u, v = (item[q][i][0] for i in (a, b, c, d))
                        if M[s][INVERSE[t]] == M[v][INVERSE[u]]:
                            pick.append((max(p0, p1), ((a, b), (c, d))))
                both.append(sorted(pick))
            tasks.append(both)
            kinds = [(0, 1)]
        else:
            kinds = [(0, 0), (0, 1), (1, 0), (1, 1)]
        for h, g in kinds:
            tasks.append(
                [sorted((p, ((a, b),)) for p, a, b in ways[(delta, h, g)][q]) for q in range(2)]
            )
    return tasks


def arrays_of(way):
    return {a for pair in way[1] for a in pair}


def assign(tasks):
    left = list(range(len(tasks)))
    phases = []
    for p, room in enumerate(TILES):
        final = p == len(TILES) - 1
        options = {
            k: [[w for w in tasks[k][q] if w[0] <= p] for q in range(2)] for k in left
        }
        options = {k: o for k, o in options.items() if o[0] or o[1]}
        if final:
            assert len(options) == len(left)
            room = -(-len(left) // 2)
        chosen, used = {}, set()
        counts = [0, 0]
        while options:
            best = None
            for k, o in options.items():
                for q in range(2):
                    if counts[q] >= room:
                        continue
                    for w in o[q]:
                        new = len(arrays_of(w) - used)
                        only = not o[1 - q]
                        rank = (not (final and only), new, counts[q], not only, k, q, w)
                        if best is None or rank < best[0]:
                            best = (rank, k, q, w)
            if best is None:
                break
            _, k, q, w = best
            chosen[k] = (q, w)
            counts[q] += 1
            used |= arrays_of(w)
            del options[k]
        assert not final or not options
        changed = True
        while changed:
            changed = False
            for a in sorted(used, key=lambda a: sum(a in arrays_of(w) for _, w in chosen.values())):
                trial = {}
                for k, (q, w) in chosen.items():
                    if a in arrays_of(w):
                        fits = [
                            v
                            for v in tasks[k][q]
                            if v[0] <= p and arrays_of(v) <= used and a not in arrays_of(v)
                        ]
                        if not fits:
                            break
                        w = fits[0]
                    trial[k] = (q, w)
                else:
                    chosen = trial
                    used = used - {a}
                    changed = True
                    break
        left = [k for k in left if k not in chosen]
        phases.append([[w for q, w in chosen.values() if q == side] for side in range(2)])
    assert not left
    return phases


def order_arrays(lists, start):
    names = sorted({a for side in lists for w in side for a in arrays_of(w)} | set(start))
    placed = list(start)
    while len(placed) < len(names):
        def score(a):
            have = set(placed) | {a}
            return sum(arrays_of(w) <= have for side in lists for w in side)

        def degree(a):
            return sum(a in arrays_of(w) for side in lists for w in side)

        placed.append(
            max((a for a in names if a not in placed), key=lambda a: (score(a), degree(a)))
        )
    return placed


def cover(lists):
    edges = [set(pair) for side in lists for w in side for pair in w[1]]
    picked = []
    while edges:
        names = sorted({a for e in edges for a in e})
        a = max(names, key=lambda n: sum(n in e for e in edges))
        picked.append(a)
        edges = [e for e in edges if a not in e]
    return picked


def make_tables():
    held = items_of_variables()
    count = 2 * len(held)
    item = [[held[a // 2][q ^ (a % 2)] for a in range(count)] for q in range(2)]
    first = [(FIRST_SWAPPED if a % 2 else FIRST)[a // 2] for a in range(count)]
    phases = assign(make_tasks(item, first))
    layout = []
    width = 0
    for p, lists in enumerate(phases):
        arrays = order_arrays(lists, [0, 1] if p == 0 else [])
        lefts = cover(lists)
        if p == 0:
            lefts = [0] + [a for a in lefts if a != 0]
        tiles = max(len(side) for side in lists)
        tiles = -(-tiles // UNROLL) * UNROLL
        layout.append([arrays, lefts, tiles, 2 if p == 0 else 1, width])
        width += 4 * tiles + tiles // UNROLL
    owners_at = width
    width += count
    table = np.zeros((128, width), np.int32)
    for chip in CHIPS:
        for q in range(2):
            line = table[device_of(chip, q)]
            for entry, lists in zip(layout, phases):
                arrays, lefts, tiles, _, at = entry
                place = {a: i for i, a in enumerate(arrays)}
                acc = {a: i for i, a in enumerate(lefts)}
                picked = []
                for _, pairs in lists[q]:
                    a, b = pairs[0]
                    t, s = (M[chip][item[q][i][0]] for i in (a, b))
                    if len(pairs) == 2 and t > s:
                        a, b = pairs[1]
                    if a not in acc:
                        a, b = b, a
                    picked.append((place[a], place[b], acc[a], place[b]))
                picked.sort(key=lambda u: max(u[:2]))
                for u in range(tiles):
                    line[at + 4 * u : at + 4 * u + 4] = (
                        picked[u] if u < len(picked) else (0, 0, len(lefts), len(arrays))
                    )
                for v in range(tiles // UNROLL):
                    part = picked[: (v + 1) * UNROLL]
                    line[at + 4 * tiles + v] = 1 + max([max(u[:2]) for u in part] + [0])
                if at:
                    entry[3] = max(entry[3], int(line[at + 4 * tiles]))
            for a, (t, h) in enumerate(item[q]):
                line[owners_at + a] = device_of(M[chip][t], h)
    return layout, owners_at, table


def cubed(left, right):
    inner = lax.dot_general(
        left, right, (((1,), (1,)), ((), ())), preferred_element_type=jnp.float32
    )
    shifted = inner + float(WIDTH)
    return shifted * shifted * shifted


def tile_kernel(phase, layout, owners_at, total, *refs):
    arrays, lefts, tiles, wave, at = layout[phase]
    last = phase == len(layout) - 1
    n = len(arrays)
    table = refs[0]
    sources = refs[1 : 1 + n]
    earlier = refs[1 + n : 1 + n + phase] if last else ()
    out, rows, row_sums, col_sums, sems = refs[-5:]

    def fetch(begin, end):
        for i in range(begin, end):
            pltpu.make_async_copy(sources[i], rows.at[i], sems.at[i]).start()

    fetch(0, wave)
    row_sums[...] = jnp.zeros_like(row_sums)
    col_sums[...] = jnp.zeros_like(col_sums)
    out[...] = jnp.zeros_like(out)

    def wait_for(i, carry):
        pltpu.make_async_copy(sources[0], rows.at[i], sems.at[i]).wait()
        return carry

    def add_rows(i, p):
        row_sums[i, 0] += p[:, :128]
        row_sums[i, 1] += p[:, 128:]

    ready = 0
    if phase == 0:
        ready = 2
        lax.fori_loop(0, 2, wait_for, 0)
        fetch(wave, n)
        left = rows[0]
        p = cubed(left, left)
        i0 = lax.broadcasted_iota(jnp.int32, p.shape, 0)
        i1 = lax.broadcasted_iota(jnp.int32, p.shape, 1)
        add_rows(0, jnp.where(i0 == i1, 0.0, p))
        add_rows(0, cubed(left, rows[1]))

    else:
        ready = wave
        lax.fori_loop(0, wave, wait_for, 0)
        fetch(wave, n)

    def some_tiles(v, ready):
        need = jnp.maximum(table[at + 4 * tiles + v], ready)
        lax.fori_loop(ready, need, wait_for, 0)
        for j in range(UNROLL):
            u = at + 4 * (v * UNROLL + j)
            p = cubed(rows[table[u]], rows[table[u + 1]])
            add_rows(table[u + 2], p)
            c = table[u + 3]
            col_sums[c, 0] += jnp.sum(p[:128].reshape(16, 8, 256), axis=0)
            col_sums[c, 1] += jnp.sum(p[128:].reshape(16, 8, 256), axis=0)
        return need

    ready = lax.fori_loop(0, tiles // UNROLL, some_tiles, jnp.int32(ready))
    lax.fori_loop(ready, n, wait_for, 0)

    same = 1.0 / ((ROWS - 1.0) * WIDTH**3)
    cross = -1.0 / (float(ROWS) * WIDTH**3)
    sums = {}
    for i, a in enumerate(arrays):
        c0, c1 = col_sums[i, 0], col_sums[i, 1]
        eight = jnp.concatenate(
            [
                same * c0[:, :128] + cross * c1[:, :128],
                cross * c0[:, 128:] + same * c1[:, 128:],
            ],
            axis=1,
        )
        if a in lefts:
            k = lefts.index(a)
            r0, r1 = row_sums[k, 0], row_sums[k, 1]
            top = same * r0[:128] + cross * r1[:128]
            low = cross * r0[128:] + same * r1[128:]
            r = jnp.concatenate([top.T, low.T], axis=1)
            eight = eight + jnp.sum(r.reshape(16, 8, 256), axis=0)
        sums[a] = jnp.sum(eight, axis=0, keepdims=True)
    if not last:
        for a in arrays:
            out[a : a + 1, :] = sums[a]
        return
    everything = jnp.zeros((1, 128), jnp.float32)
    for a in range(total):
        s = sums.get(a, jnp.zeros((1, 256), jnp.float32))
        for e in earlier:
            s = s + e[a : a + 1, :]
        everything = everything + s[:, :128] + s[:, 128:]
        out[table[owners_at + a], :, 0:256] = s
    out[:, :, 256:384] = jnp.broadcast_to(everything[None], (128, 1, 128))


def run_phase(phase, layout, owners_at, total, table, values, earlier):
    arrays, lefts, tiles, _, _ = layout[phase]
    last = phase == len(layout) - 1
    n = len(arrays)
    vmem = pl.BlockSpec(memory_space=pltpu.VMEM)
    shape = (128, 1, 384) if last else (-(-total // 8) * 8, 256)
    return pl.pallas_call(
        functools.partial(tile_kernel, phase, layout, owners_at, total),
        out_shape=jax.ShapeDtypeStruct(shape, jnp.float32),
        in_specs=[pl.BlockSpec(memory_space=pltpu.SMEM)]
        + [pl.BlockSpec(memory_space=pl.ANY)] * n
        + [vmem] * (phase if last else 0),
        out_specs=vmem,
        scratch_shapes=[
            pltpu.VMEM((n, 256, WIDTH), jnp.bfloat16),
            pltpu.VMEM((len(lefts) + 1, 2, 256, 128), jnp.float32),
            pltpu.VMEM((n + 1, 2, 8, 256), jnp.float32),
            pltpu.SemaphoreType.DMA((n,)),
        ],
        compiler_params=pltpu.CompilerParams(vmem_limit_bytes=56 * 2**20),
        cost_estimate=pl.CostEstimate(
            flops=tiles * 2 * 256 * 256 * WIDTH, bytes_accessed=n * 2**20, transcendentals=0
        ),
    )(table, *[values[a] for a in arrays], *(earlier if last else ()))


def hop(value, step0, step1):
    pairs = []
    for chip in CHIPS:
        for q, s in enumerate((step0, step1)):
            pairs.append((device_of(M[chip][STEPS[s]], q), device_of(chip, q)))
    return lax.ppermute(value, AXES, pairs)


def swap(value):
    return lax.ppermute(
        value, AXES, [(device_of(c, q), device_of(c, 1 - q)) for c in CHIPS for q in range(2)]
    )


def shards(layout, owners_at, table, real_feats, fake_feats):
    me = lax.axis_index(AXES)
    mine = lax.dynamic_index_in_dim(jnp.asarray(table), me, 0, keepdims=False)
    own = jnp.concatenate([real_feats, fake_feats], axis=0)
    needed = swaps_needed(layout)
    values = {0: own}
    for v in range(len(HOPS) + 1):
        if v:
            source, swapped, step0, step1 = HOPS[v - 1]
            values[2 * v] = hop(values[2 * source + swapped], step0, step1)
        if 2 * v + 1 in needed:
            values[2 * v + 1] = swap(values[2 * v])
    total = 2 * len(HOPS) + 2
    parts = []
    for phase in range(len(layout)):
        parts.append(run_phase(phase, layout, owners_at, total, mine, values, parts))
    received = lax.all_to_all(parts[-1], AXES, 0, 0, tiled=True)
    sums = jnp.sum(received, axis=(0, 1))
    return sums[:128], sums[128:256], jnp.sum(sums[256:]) / float(ROWS)


def swaps_needed(layout):
    needed = {a for arrays, *_ in layout for a in arrays if a % 2}
    return needed | {2 * s + 1 for s, w, _, _ in HOPS if w}


def solution(mesh):
    layout, owners_at, table = make_tables()
    placed = P(AXES, None)

    def body(real_feats, fake_feats):
        return shards(layout, owners_at, table, real_feats, fake_feats)

    return jax.shard_map(
        body,
        mesh=mesh,
        in_specs=(placed, placed),
        out_specs=(P(AXES), P(AXES), P()),
        check_vma=False,
    )
```
